32 devices in a mesh: sec: 16 (over z, y, x), node: 2 (over core).
Axes of the slice: x: 2, y: 2, z: 4, core: 2. Of those that a mesh axis runs over, the one named last changes fastest.
Arguments:
- env_blocks: bfloat16 [2, 6144, 128, 128], P('node', 'sec'), may hold values from -10 to 10, as said below
- iso_blocks: bfloat16 [2, 6144, 128, 128], P('node', 'sec'), may hold values from -6 to 6
- joined_sector: int32 [2, 6144], P('node', 'sec'), may hold values from 0 to 15, as said below
- owner_map: int32 [2, 16], P('node'), may hold values from 0 to 15, each once within a row
- live_pairs: int32 [2, 16], P('node', 'sec'), may hold values from 1 to 384, as said below
Outputs:
- environment: float32 [2, 16, 128, 128], P('node', 'sec')
The draws below stay inside these ranges and needn't reach their ends.
Inputs may be any that keep to these rules, and one draw needn't show every extreme that they name: `env_blocks`: each block is symmetric. `joined_sector`: slot p belongs to tree node k = p // 3072 of its group, and its sector is one of that node's sectors k * 8 to k * 8 + 7. `owner_map`: each row names every index once. `live_pairs`: in every group some index of sec has all 384 slots live.
All inputs are finite; a program needn't handle non-finite values.
Results may differ from the reference program's by a relative error of at most 0.0003.
Values sent between devices are 32-bit elements; how exact they have to be, the bound alone decides.
A program may use at most 128 MiB of HBM per device.

```python
import math
import jax
import jax.numpy as jnp
from jax import lax

R = 128
DC = 128
SECTORS_NODE = 8
PAIRS_DEV = 384
NODES = 2
SECTORS = 16
PAIRS = 6144


def draw_env_blocks(key, part):
    base = jax.random.truncated_normal(jax.random.fold_in(key, 11), -4.0, 4.0, (NODES, PAIRS, R, R), jnp.float32)
    blocks = (base + jnp.swapaxes(base, -1, -2)) * (0.7 / math.sqrt(R)) + jnp.eye(R, dtype=jnp.float32)
    return blocks.astype(jnp.bfloat16)


def draw_iso_blocks(key, part):
    tree_count = PAIRS // (PAIRS_DEV * SECTORS_NODE)
    per_tree = PAIRS_DEV * SECTORS_NODE
    shared = jax.random.truncated_normal(jax.random.fold_in(key, 41), -4.0, 4.0, (NODES, tree_count, 1, R, DC), jnp.float32)
    logs = jax.random.uniform(jax.random.fold_in(key, 42), (NODES, tree_count, 1, 1, DC), jnp.float32, math.log(0.4), math.log(4.0))
    column_scales = jnp.exp(logs)
    own = jax.random.truncated_normal(jax.random.fold_in(key, 44), -4.0, 4.0, (NODES, tree_count, per_tree, R, DC), jnp.float32)
    mixed = 0.8 * shared + 0.6 * own
    blocks = mixed * column_scales * (1.0 / math.sqrt(R))
    return blocks.reshape(NODES, PAIRS, R, DC).astype(jnp.bfloat16)


def draw_joined_sector(key, part):
    first_draw = jax.random.randint(jax.random.fold_in(key, 31), (NODES, PAIRS), 0, SECTORS_NODE)
    second_draw = jax.random.randint(jax.random.fold_in(key, 32), (NODES, PAIRS), 0, SECTORS_NODE)
    within = jnp.minimum(first_draw, second_draw)
    slots = jnp.arange(PAIRS, dtype=jnp.int32)[None, :]
    tree_node = slots // (PAIRS_DEV * SECTORS_NODE)
    return (tree_node * SECTORS_NODE + within).astype(jnp.int32)


def draw_live_pairs(key, part):
    first_draw = jax.random.randint(jax.random.fold_in(key, 21), (NODES, SECTORS), 1, PAIRS_DEV + 1)
    second_draw = jax.random.randint(jax.random.fold_in(key, 22), (NODES, SECTORS), 1, PAIRS_DEV + 1)
    counts = jnp.minimum(first_draw, second_draw)
    chosen = jax.random.randint(jax.random.fold_in(key, 23), (NODES, 1), 0, SECTORS)
    places = jnp.arange(SECTORS, dtype=jnp.int32)[None, :]
    return jnp.where(places == chosen, PAIRS_DEV, counts).astype(jnp.int32)


def setup_inputs(seed: int = 0) -> dict:
    key_list = jax.random.split(jax.random.key(seed), 6)
    return {
        "env_blocks": draw_env_blocks(jax.random.fold_in(key_list[5], 71), 0),
        "iso_blocks": draw_iso_blocks(jax.random.fold_in(key_list[5], 71), 0),
        "joined_sector": draw_joined_sector(jax.random.fold_in(key_list[5], 71), 0),
        "owner_map": jax.vmap(lambda own: jax.random.permutation(own, SECTORS))(jax.random.split(key_list[3], NODES)).reshape((NODES, SECTORS)).astype(jnp.int32),
        "live_pairs": draw_live_pairs(jax.random.fold_in(key_list[5], 71), 0),
    }


def reference(env_blocks, iso_blocks, joined_sector, owner_map, live_pairs):
    hermitians = []
    for node_index in range(NODES):
        targets_all = owner_map[node_index][joined_sector[node_index]].astype(jnp.int32)

        def one_source(partial_value, source, node_index=node_index, targets_all=targets_all):
            first_pair = (source * PAIRS_DEV).astype(jnp.int32)
            zero_index = jnp.zeros((), jnp.int32)
            node_start = (zero_index + node_index).astype(jnp.int32)
            blocks = lax.dynamic_slice(env_blocks, (node_start, first_pair, zero_index, zero_index), (1, PAIRS_DEV, R, R))[0].astype(jnp.float32)
            weights = lax.dynamic_slice(iso_blocks, (node_start, first_pair, zero_index, zero_index), (1, PAIRS_DEV, R, DC))[0].astype(jnp.float32)
            product = jnp.einsum('prk,pkc->prc', blocks, weights, precision=lax.Precision.HIGHEST).astype(jnp.bfloat16)
            sandwich = jnp.einsum('prc,prd->pcd', weights, product.astype(jnp.float32), precision=lax.Precision.HIGHEST)
            living = jnp.arange(PAIRS_DEV, dtype=jnp.int32) < live_pairs[node_index, source]
            sandwich = jnp.where(living[:, None, None], sandwich, jnp.zeros((), jnp.float32))
            targets = lax.dynamic_slice_in_dim(targets_all, first_pair, PAIRS_DEV, 0)
            return (partial_value.at[targets].add(sandwich), None)
        zero_sums = jnp.zeros((SECTORS, DC, DC), jnp.float32)
        partial_value, unused = lax.scan(one_source, zero_sums, jnp.arange(SECTORS, dtype=jnp.int32))
        hermitian = jnp.triu(partial_value) + jnp.swapaxes(jnp.triu(partial_value, 1), 1, 2)
        hermitians.append(hermitian)
    stacked = jnp.stack(hermitians, axis=0)
    grand_total = jnp.sum(stacked * stacked)
    factor = lax.rsqrt(grand_total / (NODES * SECTORS * DC * DC) + 1e-06)
    return stacked * factor
```

```python
import functools
import jax
import jax.numpy as jnp
from jax import lax
from jax.experimental import pallas as pl
from jax.experimental.pallas import tpu as pltpu
from jax.sharding import PartitionSpec as P

SECTORS_NODE = 8
CHUNK = 16
AHEAD = 6
UNROLL = 8
MESH = pl.DeviceIdType.MESH


def local_kernel(live_ref, sector_ref, env_ref, iso_ref, out_ref, blocks, weights, sums, sems):
    width = sums.shape[-1]
    half = width // 2
    live = live_ref[0, 0]
    chunks = (live + CHUNK - 1) // CHUNK

    def copies(index):
        where = pl.ds(index * CHUNK, CHUNK)
        return (
            pltpu.make_async_copy(env_ref.at[0, where], blocks.at[where], sems.at[0, index]),
            pltpu.make_async_copy(iso_ref.at[0, where], weights.at[where], sems.at[1, index]),
        )

    def start(index, carry):
        for copy in copies(index):
            copy.start()
        return carry

    lax.fori_loop(0, jnp.minimum(chunks, AHEAD), start, 0)
    sums[...] = jnp.zeros_like(sums)

    def step(index, carry):
        @pl.when(index + AHEAD < chunks)
        def _():
            start(index + AHEAD, 0)

        for copy in copies(index):
            copy.wait()

        def some(part, carry):
            first = index * CHUNK + part * UNROLL
            terms = []
            for k in range(UNROLL):
                w = weights[first + k]
                z = jnp.dot(blocks[first + k], w, preferred_element_type=jnp.float32)
                y = lax.dot_general(
                    w,
                    z.astype(jnp.bfloat16),
                    (((0,), (0,)), ((), ())),
                    preferred_element_type=jnp.float32,
                )
                terms.append(y)
            for k in range(UNROLL):
                slot = first + k
                local = lax.rem(sector_ref[0, slot], SECTORS_NODE)
                place = jnp.where(slot < live, local, SECTORS_NODE)
                sums[place] += terms[k]
            return carry

        return lax.fori_loop(0, CHUNK // UNROLL, some, carry)

    lax.fori_loop(0, chunks, step, 0)

    rows = lax.broadcasted_iota(jnp.int32, (half, width), 0)
    lanes = lax.broadcasted_iota(jnp.int32, (half, width), 1)
    piece = half // SECTORS_NODE
    for s in range(SECTORS_NODE):
        whole = sums[s]
        low = pltpu.roll(whole.T[half:], half, 1)
        packed = jnp.where(lanes >= rows, whole[:half], low)
        diagonal = jnp.sum(
            jnp.where(lanes == rows + half, whole[half:], 0.0), axis=0, keepdims=True
        )
        for c in range(SECTORS_NODE):
            out_ref[c, pl.ds(s * piece, piece)] = packed[c * piece : (c + 1) * piece]
            out_ref[c, pl.ds(half + s, 1)] = diagonal


def exchange_kernel(sec_count, node_count, owner_ref, part_ref, out_ref, first, mine, second,
                    squares, send_one, recv_one, send_two, recv_two, send_sq, recv_sq):
    members = SECTORS_NODE
    width = out_ref.shape[-1]
    half = width // 2
    piece = half // members
    me = lax.axis_index("sec")
    node = lax.axis_index("node")
    base = (me // members) * members
    rank = me - base

    barrier = pltpu.get_barrier_semaphore()
    for o in range(node_count):
        other = lax.rem(node + o, node_count)

        def greet(step, carry, other=other):
            pl.semaphore_signal(
                barrier, inc=1, device_id=(lax.rem(me + step, sec_count), other),
                device_id_type=MESH,
            )
            return carry

        lax.fori_loop(1 if o == 0 else 0, sec_count, greet, 0)
    pl.semaphore_wait(barrier, sec_count * node_count - 1)

    def to_member(step):
        peer = lax.rem(rank + step, members)
        source = lax.rem(rank + members - step, members)
        return peer, source

    def copy_one(slot, peer, step):
        return pltpu.make_async_remote_copy(
            src_ref=part_ref.at[peer], dst_ref=first.at[slot],
            send_sem=send_one.at[step], recv_sem=recv_one.at[slot],
            device_id=(base + peer, node), device_id_type=MESH,
        )

    for step in range(1, members):
        peer, _ = to_member(step)
        copy_one(step, peer, step).start()
    total = part_ref[rank]
    for step in range(1, members):
        peer, _ = to_member(step)
        copy_one(step, peer, step).wait_recv()
        total += first[step]

    shape = (half, width)
    rows = lax.rem(lax.broadcasted_iota(jnp.int32, shape, 0), piece) + rank * piece
    lanes = lax.broadcasted_iota(jnp.int32, shape, 1)
    body = total[:half]
    diagonals = total[half:]
    weight = jnp.where(lanes == rows, 1.0, 2.0)
    tall = lax.broadcasted_iota(jnp.int32, diagonals.shape, 1) - half
    here = (tall >= rank * piece) & (tall < (rank + 1) * piece)
    square = jnp.sum(weight * body * body) + jnp.sum(
        jnp.where(here, diagonals * diagonals, 0.0)
    )
    squares[me * node_count + node] = jnp.full(squares.shape[1:], square, jnp.float32)

    def copy_square(step, o):
        other = lax.rem(node + o, node_count)
        target = lax.rem(me + step, sec_count)
        place = me * node_count + node
        return pltpu.make_async_remote_copy(
            src_ref=squares.at[place], dst_ref=squares.at[place],
            send_sem=send_sq.at[o, step], recv_sem=recv_sq.at[o, step],
            device_id=(target, other), device_id_type=MESH,
        )

    for o in range(node_count):

        def send_square(step, carry, o=o):
            copy_square(step, o).start()
            return carry

        lax.fori_loop(1 if o == 0 else 0, sec_count, send_square, 0)

    def copy_two(step):
        target = lax.rem(me + step, sec_count)
        return pltpu.make_async_remote_copy(
            src_ref=mine.at[target], dst_ref=second.at[me],
            send_sem=send_two.at[step], recv_sem=recv_two.at[step],
            device_id=(target, node), device_id_type=MESH,
        )

    def fill(step, carry):
        target = lax.rem(me + step, sec_count)
        band = jnp.zeros((piece, width), jnp.float32)
        line = jnp.zeros((1, width), jnp.float32)
        for s in range(members):
            hit = jnp.full((piece, width), owner_ref[0, base + s], jnp.int32) == target
            band = jnp.where(hit, body[s * piece : (s + 1) * piece], band)
            line = jnp.where(hit[:1], diagonals[s : s + 1], line)
        mine[target, pl.ds(0, piece)] = band
        mine[target, pl.ds(piece, 1)] = line

        @pl.when(step > 0)
        def _():
            copy_two(step).start()

        return carry

    lax.fori_loop(0, sec_count, fill, 0)
    second[me] = mine[me]

    def take(step, carry):
        copy_two(step).wait_recv()
        return carry

    lax.fori_loop(1, sec_count, take, 0)
    for o in range(node_count):

        def take_square(step, carry, o=o):
            copy_square(step, o).wait_recv()
            return carry

        lax.fori_loop(1 if o == 0 else 0, sec_count, take_square, 0)

    everything = squares[:, :1, :]
    grand = jnp.sum(everything, axis=0)
    factor = lax.rsqrt(grand / (sec_count * node_count * width * width) + 1e-06)
    arrived = []
    for c in range(members):
        whole = second[c]
        for g in range(1, sec_count // members):
            whole += second[g * members + c]
        arrived.append(whole)
    packed = jnp.concatenate([a[:piece] for a in arrived], axis=0)
    diagonal = arrived[0][piece : piece + 1]
    square_form = jnp.concatenate([packed, pltpu.roll(packed, half, 1)], axis=0)
    i = lax.broadcasted_iota(jnp.int32, (width, width), 0)
    j = lax.broadcasted_iota(jnp.int32, (width, width), 1)
    kept = ((i < half) & (j >= i)) | ((j >= half) & (j < i))
    full = jnp.where(kept, square_form, square_form.T)
    full = jnp.where((i == j) & (i >= half), diagonal, full)
    out_ref[0, 0] = full * factor

    for step in range(1, members):
        peer, _ = to_member(step)
        copy_one(step, peer, step).wait_send()

    def sent(step, carry):
        copy_two(step).wait_send()
        return carry

    lax.fori_loop(1, sec_count, sent, 0)
    for o in range(node_count):

        def sent_square(step, carry, o=o):
            copy_square(step, o).wait_send()
            return carry

        lax.fori_loop(1 if o == 0 else 0, sec_count, sent_square, 0)


def local_sums(live_pairs, joined_sector, env_blocks, iso_blocks):
    pairs = env_blocks.shape[1]
    height = env_blocks.shape[2]
    width = iso_blocks.shape[3]
    half = width // 2
    chunks = pairs // CHUNK
    hbm = pl.BlockSpec(memory_space=pl.ANY)
    smem = pl.BlockSpec(memory_space=pltpu.SMEM)
    return pl.pallas_call(
        local_kernel,
        out_shape=jax.ShapeDtypeStruct((SECTORS_NODE, half + SECTORS_NODE, width), jnp.float32),
        in_specs=[smem, smem, hbm, hbm],
        out_specs=pl.BlockSpec(memory_space=pltpu.VMEM),
        scratch_shapes=[
            pltpu.VMEM((pairs, height, height), jnp.bfloat16),
            pltpu.VMEM((pairs, height, width), jnp.bfloat16),
            pltpu.VMEM((SECTORS_NODE + 1, width, width), jnp.float32),
            pltpu.SemaphoreType.DMA((2, chunks)),
        ],
        compiler_params=pltpu.CompilerParams(vmem_limit_bytes=62 * 1024 * 1024),
        name="local_sums",
    )(live_pairs, joined_sector, env_blocks, iso_blocks)


def body(env_blocks, iso_blocks, joined_sector, owner_map, live_pairs):
    width = iso_blocks.shape[3]
    half = width // 2
    piece = half // SECTORS_NODE
    sec_count = lax.axis_size("sec")
    node_count = lax.axis_size("node")
    parts = local_sums(live_pairs, joined_sector, env_blocks, iso_blocks)
    vmem = pl.BlockSpec(memory_space=pltpu.VMEM)
    dma = pltpu.SemaphoreType.DMA
    return pl.pallas_call(
        functools.partial(exchange_kernel, sec_count, node_count),
        out_shape=jax.ShapeDtypeStruct((1, 1, width, width), jnp.float32),
        in_specs=[pl.BlockSpec(memory_space=pltpu.SMEM), vmem],
        out_specs=vmem,
        scratch_shapes=[
            pltpu.VMEM(parts.shape, jnp.float32),
            pltpu.VMEM((sec_count, 2 * piece, width), jnp.float32),
            pltpu.VMEM((sec_count, 2 * piece, width), jnp.float32),
            pltpu.VMEM((sec_count * node_count, 8, width), jnp.float32),
            dma((SECTORS_NODE,)),
            dma((SECTORS_NODE,)),
            dma((sec_count,)),
            dma((sec_count,)),
            dma((node_count, sec_count)),
            dma((node_count, sec_count)),
        ],
        compiler_params=pltpu.CompilerParams(
            collective_id=0, has_side_effects=True, vmem_limit_bytes=8 * 1024 * 1024
        ),
        name="exchange",
    )(owner_map, parts)


def solution(mesh):
    in_specs = (
        P("node", "sec", None, None),
        P("node", "sec", None, None),
        P("node", "sec"),
        P("node", None),
        P("node", "sec"),
    )
    out_specs = P("node", "sec", None, None)
    return jax.shard_map(body, mesh=mesh, in_specs=in_specs, out_specs=out_specs, check_vma=False)
```

```python
import functools
import jax
import jax.numpy as jnp
from jax import lax
from jax.experimental import pallas as pl
from jax.experimental.pallas import tpu as pltpu
from jax.sharding import PartitionSpec as P

SECTORS_NODE = 8
CHUNK = 32
AHEAD = 4
MESH = pl.DeviceIdType.MESH


def local_kernel(live_ref, sector_ref, env_ref, iso_ref, out_ref, blocks, weights, held, sums, sems):
    width = sums.shape[-1]
    half = width // 2
    live = live_ref[0, 0]
    chunks = (live + CHUNK - 1) // CHUNK

    def copies(index):
        where = pl.ds(index * CHUNK, CHUNK)
        return (
            pltpu.make_async_copy(env_ref.at[0, where], blocks.at[where], sems.at[0, index]),
            pltpu.make_async_copy(iso_ref.at[0, where], weights.at[where], sems.at[1, index]),
        )

    def start(index, carry):
        for copy in copies(index):
            copy.start()
        return carry

    lax.fori_loop(0, jnp.minimum(chunks, AHEAD), start, 0)
    sums[...] = jnp.zeros_like(sums)

    pairs = CHUNK // 2
    zero = jnp.zeros(weights.shape[1:], jnp.bfloat16)

    def diagonal_pair(top, bottom):
        return jnp.concatenate(
            [jnp.concatenate([top, zero], axis=1), jnp.concatenate([zero, bottom], axis=1)],
            axis=0,
        )

    def product(index, k):
        one = index * CHUNK + 2 * k
        two = one + 1
        z = jnp.dot(
            jnp.concatenate([blocks[one], blocks[two]], axis=1),
            diagonal_pair(weights[one], weights[two]),
            preferred_element_type=jnp.float32,
        )
        held[k] = z.astype(jnp.bfloat16)

    def sandwich(index, k):
        one = index * CHUNK + 2 * k
        two = one + 1
        y = lax.dot_general(
            jnp.concatenate([weights[one], weights[two]], axis=0),
            diagonal_pair(held[k, :, :width], held[k, :, width:]),
            (((0,), (0,)), ((), ())),
            preferred_element_type=jnp.float32,
        )
        for slot, term in ((one, y[:, :width]), (two, y[:, width:])):
            local = lax.rem(sector_ref[0, slot], SECTORS_NODE)
            place = jnp.where(slot < live, local, SECTORS_NODE)
            sums[place] += term

    def arrive(index):
        @pl.when(index + AHEAD < chunks)
        def _():
            start(index + AHEAD, 0)

        for copy in copies(index):
            copy.wait()

    def step(index, carry):
        arrive(index)
        for k in range(pairs):
            sandwich(index - 1, k)
            product(index, k)
        return carry

    arrive(0)
    for k in range(pairs):
        product(0, k)
    lax.fori_loop(1, chunks, step, 0)
    for k in range(pairs):
        sandwich(chunks - 1, k)

    rows = lax.broadcasted_iota(jnp.int32, (half, width), 0)
    lanes = lax.broadcasted_iota(jnp.int32, (half, width), 1)
    piece = half // SECTORS_NODE
    for s in range(SECTORS_NODE):
        whole = sums[s]
        low = pltpu.roll(whole.T[half:], half, 1)
        packed = jnp.where(lanes >= rows, whole[:half], low)
        diagonal = jnp.sum(
            jnp.where(lanes == rows + half, whole[half:], 0.0), axis=0, keepdims=True
        )
        for c in range(SECTORS_NODE):
            out_ref[c, pl.ds(s * piece, piece)] = packed[c * piece : (c + 1) * piece]
            out_ref[c, pl.ds(half + s, 1)] = diagonal


def exchange_kernel(sec_count, node_count, owner_ref, part_ref, out_ref, first, bands, mine, second,
                    squares, picks, send_one, recv_one, send_two, recv_two, send_sq, recv_sq):
    members = SECTORS_NODE
    width = out_ref.shape[-1]
    half = width // 2
    piece = half // members
    me = lax.axis_index("sec")
    node = lax.axis_index("node")
    base = (me // members) * members
    rank = me - base

    barrier = pltpu.get_barrier_semaphore()
    for o in range(node_count):
        other = lax.rem(node + o, node_count)

        def greet(step, carry, other=other):
            pl.semaphore_signal(
                barrier, inc=1, device_id=(lax.rem(me + step, sec_count), other),
                device_id_type=MESH,
            )
            return carry

        lax.fori_loop(1 if o == 0 else 0, sec_count, greet, 0)

    def pick(target, carry):
        found = jnp.int32(members)
        for s in range(members):
            found = jnp.where(owner_ref[0, base + s] == target, s, found)
        picks[target] = found
        return carry

    lax.fori_loop(0, sec_count, pick, 0)
    pl.semaphore_wait(barrier, sec_count * node_count - 1)

    def copy_one(step):
        peer = lax.rem(rank + step, members)
        return pltpu.make_async_remote_copy(
            src_ref=part_ref.at[peer], dst_ref=first.at[step],
            send_sem=send_one.at[step], recv_sem=recv_one.at[step],
            device_id=(base + peer, node), device_id_type=MESH,
        )

    for step in range(1, members):
        copy_one(step).start()
    total = part_ref[rank]
    for step in range(1, members):
        copy_one(step).wait_recv()
        total += first[step]

    shape = (half, width)
    rows = lax.rem(lax.broadcasted_iota(jnp.int32, shape, 0), piece) + rank * piece
    lanes = lax.broadcasted_iota(jnp.int32, shape, 1)
    body = total[:half]
    diagonals = total[half:]
    weight = jnp.where(lanes == rows, 1.0, 2.0)
    tall = lax.broadcasted_iota(jnp.int32, diagonals.shape, 1) - half
    here = (tall >= rank * piece) & (tall < (rank + 1) * piece)
    weighted = weight * body * body
    folded = jnp.where(here, diagonals * diagonals, 0.0)
    for s in range(members):
        folded += weighted[s * piece : (s + 1) * piece]
    square = jnp.sum(folded, axis=0, keepdims=True)
    for s in range(members):
        bands[s, pl.ds(0, piece)] = body[s * piece : (s + 1) * piece]
        bands[s, pl.ds(piece, 1)] = diagonals[s : s + 1]
        bands[s, pl.ds(piece + 1, 1)] = square
    bands[members, pl.ds(0, piece + 1)] = jnp.zeros((piece + 1, width), jnp.float32)
    bands[members, pl.ds(piece + 1, 1)] = square

    def copy_two(step):
        target = lax.rem(me + step, sec_count)
        return pltpu.make_async_remote_copy(
            src_ref=mine.at[target], dst_ref=second.at[me],
            send_sem=send_two.at[step], recv_sem=recv_two.at[step],
            device_id=(target, node), device_id_type=MESH,
        )

    def copy_square(step, o):
        return pltpu.make_async_remote_copy(
            src_ref=bands.at[members, pl.ds(piece, 8)], dst_ref=squares.at[o - 1, me],
            send_sem=send_sq.at[o - 1, step], recv_sem=recv_sq.at[o - 1, step],
            device_id=(lax.rem(me + step, sec_count), lax.rem(node + o, node_count)),
            device_id_type=MESH,
        )

    def fill(back, carry):
        step = sec_count - 1 - back
        target = lax.rem(me + step, sec_count)
        mine[target] = bands[picks[target]]

        @pl.when(step > 0)
        def _():
            copy_two(step).start()

        for o in range(1, node_count):
            copy_square(step, o).start()
        return carry

    lax.fori_loop(0, sec_count, fill, 0)
    second[me] = mine[me]

    def take(step, carry):
        copy_two(step).wait_recv()
        return carry

    lax.fori_loop(1, sec_count, take, 0)

    arrived = []
    for c in range(members):
        whole = second[c]
        for g in range(1, sec_count // members):
            whole += second[g * members + c]
        arrived.append(whole)
    packed = jnp.concatenate([a[:piece] for a in arrived], axis=0)
    diagonal = arrived[0][piece : piece + 1]
    grand = arrived[0][piece + 1 : piece + 2]
    for c in range(1, members):
        grand += arrived[c][piece + 1 : piece + 2]
    square_form = jnp.concatenate([packed, pltpu.roll(packed, half, 1)], axis=0)
    i = lax.broadcasted_iota(jnp.int32, (width, width), 0)
    j = lax.broadcasted_iota(jnp.int32, (width, width), 1)
    kept = ((i < half) & (j >= i)) | ((j >= half) & (j < i))
    full = jnp.where(kept, square_form, square_form.T)
    full = jnp.where((i == j) & (i >= half), diagonal, full)

    for o in range(1, node_count):

        def take_square(step, carry, o=o):
            copy_square(step, o).wait_recv()
            return carry

        lax.fori_loop(0, sec_count, take_square, 0)
        grand += jnp.sum(squares[o - 1], axis=0)[1:2]
    mean = jnp.sum(grand, axis=1, keepdims=True) / (sec_count * node_count * width * width)
    out_ref[0, 0] = full * lax.rsqrt(mean + 1e-06)

    for step in range(1, members):
        copy_one(step).wait_send()

    def sent(step, carry):
        copy_two(step).wait_send()
        return carry

    lax.fori_loop(1, sec_count, sent, 0)
    for o in range(1, node_count):

        def sent_square(step, carry, o=o):
            copy_square(step, o).wait_send()
            return carry

        lax.fori_loop(0, sec_count, sent_square, 0)


def local_sums(live_pairs, joined_sector, env_blocks, iso_blocks):
    pairs = env_blocks.shape[1]
    height = env_blocks.shape[2]
    width = iso_blocks.shape[3]
    half = width // 2
    chunks = pairs // CHUNK
    hbm = pl.BlockSpec(memory_space=pl.ANY)
    smem = pl.BlockSpec(memory_space=pltpu.SMEM)
    return pl.pallas_call(
        local_kernel,
        out_shape=jax.ShapeDtypeStruct((SECTORS_NODE, half + SECTORS_NODE, width), jnp.float32),
        in_specs=[smem, smem, hbm, hbm],
        out_specs=pl.BlockSpec(memory_space=pltpu.VMEM),
        scratch_shapes=[
            pltpu.VMEM((pairs, height, height), jnp.bfloat16),
            pltpu.VMEM((pairs, height, width), jnp.bfloat16),
            pltpu.VMEM((CHUNK // 2, height, 2 * width), jnp.bfloat16),
            pltpu.VMEM((SECTORS_NODE + 1, width, width), jnp.float32),
            pltpu.SemaphoreType.DMA((2, chunks)),
        ],
        compiler_params=pltpu.CompilerParams(vmem_limit_bytes=56 * 1024 * 1024),
        name="local_sums",
    )(live_pairs, joined_sector, env_blocks, iso_blocks)


def body(env_blocks, iso_blocks, joined_sector, owner_map, live_pairs):
    width = iso_blocks.shape[3]
    half = width // 2
    piece = half // SECTORS_NODE
    sec_count = lax.axis_size("sec")
    node_count = lax.axis_size("node")
    parts = local_sums(live_pairs, joined_sector, env_blocks, iso_blocks)
    vmem = pl.BlockSpec(memory_space=pltpu.VMEM)
    dma = pltpu.SemaphoreType.DMA
    return pl.pallas_call(
        functools.partial(exchange_kernel, sec_count, node_count),
        out_shape=jax.ShapeDtypeStruct((1, 1, width, width), jnp.float32),
        in_specs=[pl.BlockSpec(memory_space=pltpu.SMEM), vmem],
        out_specs=vmem,
        scratch_shapes=[
            pltpu.VMEM(parts.shape, jnp.float32),
            pltpu.VMEM((SECTORS_NODE + 1, piece + 8, width), jnp.float32),
            pltpu.VMEM((sec_count, piece + 8, width), jnp.float32),
            pltpu.VMEM((sec_count, piece + 8, width), jnp.float32),
            pltpu.VMEM((max(node_count - 1, 1), sec_count, 8, width), jnp.float32),
            pltpu.SMEM((sec_count,), jnp.int32),
            dma((SECTORS_NODE,)),
            dma((SECTORS_NODE,)),
            dma((sec_count,)),
            dma((sec_count,)),
            dma((max(node_count - 1, 1), sec_count)),
            dma((max(node_count - 1, 1), sec_count)),
        ],
        compiler_params=pltpu.CompilerParams(
            collective_id=0, has_side_effects=True, vmem_limit_bytes=8 * 1024 * 1024
        ),
        name="exchange",
    )(owner_map, parts)


def solution(mesh):
    in_specs = (
        P("node", "sec", None, None),
        P("node", "sec", None, None),
        P("node", "sec"),
        P("node", None),
        P("node", "sec"),
    )
    out_specs = P("node", "sec", None, None)
    return jax.shard_map(body, mesh=mesh, in_specs=in_specs, out_specs=out_specs, check_vma=False)
```

```python
import functools
import jax
import jax.numpy as jnp
from jax import lax
from jax.experimental import pallas as pl
from jax.experimental.pallas import tpu as pltpu
from jax.sharding import PartitionSpec as P

SECTORS_NODE = 8
CHUNK = 32
AHEAD = 4
MESH = pl.DeviceIdType.MESH


def local_kernel(live_ref, sector_hbm, env_ref, iso_ref, sums, blocks, weights, held, sector_ref,
                 sems, sector_sem):
    width = sums.shape[-1]
    live = live_ref[0, 0]
    chunks = (live + CHUNK - 1) // CHUNK

    def copies(index):
        where = pl.ds(index * CHUNK, CHUNK)
        return (
            pltpu.make_async_copy(env_ref.at[0, where], blocks.at[where], sems.at[0, index]),
            pltpu.make_async_copy(iso_ref.at[0, where], weights.at[where], sems.at[1, index]),
        )

    def start(index, carry):
        for copy in copies(index):
            copy.start()
        return carry

    lax.fori_loop(0, jnp.minimum(chunks, AHEAD), start, 0)
    sector_copy = pltpu.make_async_copy(sector_hbm, sector_ref, sector_sem)
    sector_copy.start()
    sums[...] = jnp.zeros_like(sums)

    pairs = CHUNK // 2
    zero = jnp.zeros(weights.shape[1:], jnp.bfloat16)

    def diagonal_pair(top, bottom):
        return jnp.concatenate(
            [jnp.concatenate([top, zero], axis=1), jnp.concatenate([zero, bottom], axis=1)],
            axis=0,
        )

    def product(index, k):
        one = index * CHUNK + 2 * k
        two = one + 1
        z = jnp.dot(
            jnp.concatenate([blocks[one], blocks[two]], axis=1),
            diagonal_pair(weights[one], weights[two]),
            preferred_element_type=jnp.float32,
        )
        held[k] = z.astype(jnp.bfloat16)

    def sandwich(index, k):
        one = index * CHUNK + 2 * k
        two = one + 1
        y = lax.dot_general(
            jnp.concatenate([weights[one], weights[two]], axis=0),
            diagonal_pair(held[k, :, :width], held[k, :, width:]),
            (((0,), (0,)), ((), ())),
            preferred_element_type=jnp.float32,
        )
        for slot, term in ((one, y[:, :width]), (two, y[:, width:])):
            local = lax.rem(sector_ref[0, slot], SECTORS_NODE)
            place = jnp.where(slot < live, local, SECTORS_NODE)
            sums[place] += term

    def arrive(index):
        @pl.when(index + AHEAD < chunks)
        def _():
            start(index + AHEAD, 0)

        for copy in copies(index):
            copy.wait()

    def step(index, carry):
        arrive(index)
        for k in range(pairs):
            sandwich(index - 1, k)
            product(index, k)
        return carry

    arrive(0)
    for k in range(pairs):
        product(0, k)
    sector_copy.wait()
    lax.fori_loop(1, chunks, step, 0)
    for k in range(pairs):
        sandwich(chunks - 1, k)


def exchange_kernel(sec_count, node_count, owner_ref, sums_ref, out_ref, part_ref, first, bands, mine, second,
                    squares, picks, send_one, recv_one, send_two, recv_two, send_sq, recv_sq):
    members = SECTORS_NODE
    width = out_ref.shape[-1]
    half = width // 2
    piece = half // members
    me = lax.axis_index("sec")
    node = lax.axis_index("node")
    base = (me // members) * members
    rank = me - base

    barrier = pltpu.get_barrier_semaphore()
    for o in range(node_count):
        other = lax.rem(node + o, node_count)

        def greet(step, carry, other=other):
            pl.semaphore_signal(
                barrier, inc=1, device_id=(lax.rem(me + step, sec_count), other),
                device_id_type=MESH,
            )
            return carry

        lax.fori_loop(1 if o == 0 else 0, sec_count, greet, 0)

    rows = lax.broadcasted_iota(jnp.int32, (half, width), 0)
    lanes = lax.broadcasted_iota(jnp.int32, (half, width), 1)
    for s in range(members):
        whole = sums_ref[s]
        low = pltpu.roll(whole.T[half:], half, 1)
        packed = jnp.where(lanes >= rows, whole[:half], low)
        diagonal = jnp.sum(
            jnp.where(lanes == rows + half, whole[half:], 0.0), axis=0, keepdims=True
        )
        for c in range(members):
            part_ref[c, pl.ds(s * piece, piece)] = packed[c * piece : (c + 1) * piece]
            part_ref[c, pl.ds(half + s, 1)] = diagonal

    def pick(target, carry):
        found = jnp.int32(members)
        for s in range(members):
            found = jnp.where(owner_ref[0, base + s] == target, s, found)
        picks[target] = found
        return carry

    lax.fori_loop(0, sec_count, pick, 0)
    pl.semaphore_wait(barrier, sec_count * node_count - 1)

    def copy_one(step):
        peer = lax.rem(rank + step, members)
        return pltpu.make_async_remote_copy(
            src_ref=part_ref.at[peer], dst_ref=first.at[step],
            send_sem=send_one.at[step], recv_sem=recv_one.at[step],
            device_id=(base + peer, node), device_id_type=MESH,
        )

    for step in range(1, members):
        copy_one(step).start()
    total = part_ref[rank]
    for step in range(1, members):
        copy_one(step).wait_recv()
        total += first[step]

    shape = (half, width)
    rows = lax.rem(lax.broadcasted_iota(jnp.int32, shape, 0), piece) + rank * piece
    lanes = lax.broadcasted_iota(jnp.int32, shape, 1)
    body = total[:half]
    diagonals = total[half:]
    weight = jnp.where(lanes == rows, 1.0, 2.0)
    tall = lax.broadcasted_iota(jnp.int32, diagonals.shape, 1) - half
    here = (tall >= rank * piece) & (tall < (rank + 1) * piece)
    weighted = weight * body * body
    folded = jnp.where(here, diagonals * diagonals, 0.0)
    for s in range(members):
        folded += weighted[s * piece : (s + 1) * piece]
    square = jnp.sum(folded, axis=0, keepdims=True)
    for s in range(members):
        bands[s, pl.ds(0, piece)] = body[s * piece : (s + 1) * piece]
        bands[s, pl.ds(piece, 1)] = diagonals[s : s + 1]
        bands[s, pl.ds(piece + 1, 1)] = square
    bands[members, pl.ds(0, piece + 1)] = jnp.zeros((piece + 1, width), jnp.float32)
    bands[members, pl.ds(piece + 1, 1)] = square

    def copy_two(step):
        target = lax.rem(me + step, sec_count)
        return pltpu.make_async_remote_copy(
            src_ref=mine.at[target], dst_ref=second.at[me],
            send_sem=send_two.at[step], recv_sem=recv_two.at[step],
            device_id=(target, node), device_id_type=MESH,
        )

    def copy_square(step, o):
        return pltpu.make_async_remote_copy(
            src_ref=bands.at[members, pl.ds(piece, 8)], dst_ref=squares.at[o - 1, me],
            send_sem=send_sq.at[o - 1, step], recv_sem=recv_sq.at[o - 1, step],
            device_id=(lax.rem(me + step, sec_count), lax.rem(node + o, node_count)),
            device_id_type=MESH,
        )

    def fill(back, carry):
        step = sec_count - 1 - back
        target = lax.rem(me + step, sec_count)
        mine[target] = bands[picks[target]]

        @pl.when(step > 0)
        def _():
            copy_two(step).start()

        for o in range(1, node_count):
            copy_square(step, o).start()
        return carry

    lax.fori_loop(0, sec_count, fill, 0)
    second[me] = mine[me]

    def take(step, carry):
        copy_two(step).wait_recv()
        return carry

    lax.fori_loop(1, sec_count, take, 0)

    arrived = []
    for c in range(members):
        whole = second[c]
        for g in range(1, sec_count // members):
            whole += second[g * members + c]
        arrived.append(whole)
    packed = jnp.concatenate([a[:piece] for a in arrived], axis=0)
    diagonal = arrived[0][piece : piece + 1]
    grand = arrived[0][piece + 1 : piece + 2]
    for c in range(1, members):
        grand += arrived[c][piece + 1 : piece + 2]
    square_form = jnp.concatenate([packed, pltpu.roll(packed, half, 1)], axis=0)
    i = lax.broadcasted_iota(jnp.int32, (width, width), 0)
    j = lax.broadcasted_iota(jnp.int32, (width, width), 1)
    kept = ((i < half) & (j >= i)) | ((j >= half) & (j < i))
    full = jnp.where(kept, square_form, square_form.T)
    full = jnp.where((i == j) & (i >= half), diagonal, full)

    for o in range(1, node_count):

        def take_square(step, carry, o=o):
            copy_square(step, o).wait_recv()
            return carry

        lax.fori_loop(0, sec_count, take_square, 0)
        grand += jnp.sum(squares[o - 1], axis=0)[1:2]
    mean = jnp.sum(grand, axis=1, keepdims=True) / (sec_count * node_count * width * width)
    out_ref[0, 0] = full * lax.rsqrt(mean + 1e-06)

    for step in range(1, members):
        copy_one(step).wait_send()

    def sent(step, carry):
        copy_two(step).wait_send()
        return carry

    lax.fori_loop(1, sec_count, sent, 0)
    for o in range(1, node_count):

        def sent_square(step, carry, o=o):
            copy_square(step, o).wait_send()
            return carry

        lax.fori_loop(0, sec_count, sent_square, 0)


def local_sums(live_pairs, joined_sector, env_blocks, iso_blocks):
    pairs = env_blocks.shape[1]
    height = env_blocks.shape[2]
    width = iso_blocks.shape[3]
    chunks = pairs // CHUNK
    hbm = pl.BlockSpec(memory_space=pltpu.HBM)
    smem = pl.BlockSpec(memory_space=pltpu.SMEM)
    return pl.pallas_call(
        local_kernel,
        out_shape=jax.ShapeDtypeStruct((SECTORS_NODE + 1, width, width), jnp.float32),
        in_specs=[smem, hbm, hbm, hbm],
        out_specs=pl.BlockSpec(memory_space=pltpu.VMEM),
        scratch_shapes=[
            pltpu.VMEM((pairs, height, height), jnp.bfloat16),
            pltpu.VMEM((pairs, height, width), jnp.bfloat16),
            pltpu.VMEM((CHUNK // 2, height, 2 * width), jnp.bfloat16),
            pltpu.SMEM(joined_sector.shape, jnp.int32),
            pltpu.SemaphoreType.DMA((2, chunks)),
            pltpu.SemaphoreType.DMA,
        ],
        compiler_params=pltpu.CompilerParams(vmem_limit_bytes=52 * 1024 * 1024),
        name="local_sums",
    )(live_pairs, joined_sector, env_blocks, iso_blocks)


def body(env_blocks, iso_blocks, joined_sector, owner_map, live_pairs):
    width = iso_blocks.shape[3]
    half = width // 2
    piece = half // SECTORS_NODE
    sec_count = lax.axis_size("sec")
    node_count = lax.axis_size("node")
    sums = local_sums(live_pairs, joined_sector, env_blocks, iso_blocks)
    vmem = pl.BlockSpec(memory_space=pltpu.VMEM)
    dma = pltpu.SemaphoreType.DMA
    return pl.pallas_call(
        functools.partial(exchange_kernel, sec_count, node_count),
        out_shape=jax.ShapeDtypeStruct((1, 1, width, width), jnp.float32),
        in_specs=[pl.BlockSpec(memory_space=pltpu.SMEM), vmem],
        out_specs=vmem,
        scratch_shapes=[
            pltpu.VMEM((SECTORS_NODE, half + SECTORS_NODE, width), jnp.float32),
            pltpu.VMEM((SECTORS_NODE, half + SECTORS_NODE, width), jnp.float32),
            pltpu.VMEM((SECTORS_NODE + 1, piece + 8, width), jnp.float32),
            pltpu.VMEM((sec_count, piece + 8, width), jnp.float32),
            pltpu.VMEM((sec_count, piece + 8, width), jnp.float32),
            pltpu.VMEM((max(node_count - 1, 1), sec_count, 8, width), jnp.float32),
            pltpu.SMEM((sec_count,), jnp.int32),
            dma((SECTORS_NODE,)),
            dma((SECTORS_NODE,)),
            dma((sec_count,)),
            dma((sec_count,)),
            dma((max(node_count - 1, 1), sec_count)),
            dma((max(node_count - 1, 1), sec_count)),
        ],
        compiler_params=pltpu.CompilerParams(
            collective_id=0, has_side_effects=True, vmem_limit_bytes=8 * 1024 * 1024
        ),
        name="exchange",
    )(owner_map, sums)


def solution(mesh):
    in_specs = (
        P("node", "sec", None, None),
        P("node", "sec", None, None),
        P("node", "sec"),
        P("node", None),
        P("node", "sec"),
    )
    out_specs = P("node", "sec", None, None)
    return jax.shard_map(body, mesh=mesh, in_specs=in_specs, out_specs=out_specs, check_vma=False)
```
